32 devices in a mesh: groups: 2 (over y), dp: 4 (over z), mp: 4 (over x, core).
Axes of the slice: x: 2, y: 2, z: 4, core: 2. Of those that a mesh axis runs over, the one named last changes fastest.
Arguments:
- hidden: bfloat16 [8, 8192], P(('groups', 'mp'), 'dp'), parts along dimension 0, may hold values from -530 to 530
- attention_gain: float32 [8192], P('dp'), may hold values from 0.25 to 1.75
- query_weight: bfloat16 [8192, 8192], P('dp', 'mp'), may hold values from -0.0625 to 0.0625
- key_projector: bfloat16 [8192, 1024], P('dp', 'mp'), may hold values from -0.0625 to 0.0625
- value_projector: bfloat16 [8192, 1024], P('dp', 'mp'), may hold values from -0.0625 to 0.0625
- out_weight: bfloat16 [8192, 8192], P('mp', 'dp'), may hold values from -0.1875 to 0.1875
- key_cache: bfloat16 [8, 8, 256, 128], P(('groups', 'dp'), 'mp'), parts along dimension 0, may hold values from -1230 to 1230
- earlier_value_cache: bfloat16 [8, 8, 256, 128], P(('groups', 'dp'), 'mp'), parts along dimension 0, may hold values from -6 to 6
- cached_length_per_row: int32 [8], P(('groups', 'dp')), parts along dimension 0, may hold values from 1 to 256
- final_gain: float32 [8192], replicated, may hold values from 0.25 to 1.75
- head_weight: bfloat16 [32000, 8192], P('dp', 'mp'), may hold values from -41 to 41
- draft_ids: int32 [8], P(('groups', 'mp')), parts along dimension 0, may hold values from 0 to 31999
Outputs:
- residual_out: bfloat16 [8, 8192], P(('groups', 'mp'), 'dp'), parts along dimension 0
- draft_logprob: float32 [8], P(('groups', 'mp')), parts along dimension 0
The draws below stay inside these ranges and needn't reach their ends.
There are 2 independent parts, one for each index of `groups`. The reference program is written for one: setup_inputs(seed, part) draws one part's arguments, and reference() takes and returns one part's arrays. A program takes and returns all parts, laid end to end along the dimension named above; an argument that names none is the same for every part. Nothing has to cross between parts.
All inputs are finite; a program needn't handle non-finite values.
Results may differ from the reference program's by a relative error of at most 0.0035.
Values may be sent and summed in bfloat16 or wider, within the bound.
A program may use at most 128 MiB of HBM per device.

```python
import math
import jax
import jax.numpy as jnp
from jax import lax

MODEL_WIDTH = 8192
QUERY_HEADS = 64
KEY_VALUE_HEADS = 8
HEAD_WIDTH = 128
VOCAB = 32000
CACHE_SLOTS = 256
SEQUENCE_COUNT = 4


def draw_hidden(key, part):
    residual_streams = jax.random.split(jax.random.fold_in(key, 11), 3)
    row_scale = jnp.exp(jax.random.uniform(residual_streams[1], (SEQUENCE_COUNT, 1), minval=math.log(0.5), maxval=math.log(5.0)))
    col_scale = jnp.exp(jax.random.uniform(residual_streams[2], (1, MODEL_WIDTH), minval=math.log(0.5), maxval=math.log(2.0)))
    position = jnp.arange(MODEL_WIDTH, dtype=jnp.float32)[None, :] / MODEL_WIDTH
    cache_entries = jax.random.truncated_normal(residual_streams[0], -6.0, 6.0, (SEQUENCE_COUNT, MODEL_WIDTH))
    return (cache_entries * row_scale * col_scale * 3.0 ** position).astype(jnp.bfloat16)


def draw_key_cache(key, part):
    residual_streams = jax.random.split(jax.random.fold_in(key, 23), 2)
    per_head_scale = jnp.exp(jax.random.uniform(residual_streams[1], (SEQUENCE_COUNT, KEY_VALUE_HEADS, 1, 1), minval=0.0, maxval=math.log(4.0)))
    cache_entries = jax.random.truncated_normal(residual_streams[0], -6.0, 6.0, (SEQUENCE_COUNT, KEY_VALUE_HEADS, CACHE_SLOTS, HEAD_WIDTH)) * per_head_scale
    return cache_entries.astype(jnp.bfloat16)


def draw_head_weight(key, part):
    residual_streams = jax.random.split(jax.random.fold_in(key, 37), 2)
    position = jnp.arange(VOCAB, dtype=jnp.float32)[:, None] / VOCAB
    row_scale = jnp.exp(jax.random.uniform(residual_streams[1], (VOCAB, 1), minval=math.log(0.5), maxval=math.log(5.0)))
    row_scale = row_scale * 3.0 ** position / math.sqrt(MODEL_WIDTH)
    cache_entries = jax.random.truncated_normal(residual_streams[0], -6.0, 6.0, (VOCAB, MODEL_WIDTH)) * row_scale
    return cache_entries.astype(jnp.bfloat16)


def set_ends(values, key, smallest, largest):
    shape = values.shape
    spot = [jax.random.randint(jax.random.fold_in(key, axis), (), 0, shape[axis]) for axis in range(len(shape))]
    values = values.at[tuple(spot)].set(smallest)
    longest = shape.index(max(shape))
    spot[longest] = (spot[longest] + 1) % shape[longest]
    return values.at[tuple(spot)].set(largest)


def steps_of(stream_key, shape, cuts, smallest, top_value):
    def one(dim, shards_of):
        draws = jax.random.uniform(jax.random.fold_in(jax.random.fold_in(stream_key, 6), dim), (shards_of,), jnp.float32, smallest / len(cuts), top_value / len(cuts))
        return jnp.repeat(jnp.exp(draws), shape[dim] // shards_of).reshape((-1,) + (1,) * (len(shape) - dim - 1))

    loudness = one(*cuts[0])
    for cut in cuts[1:]:
        loudness = loudness * one(*cut)
    return loudness


def noise(rng, dims, deviation, limit, pieces=(), kind=jnp.bfloat16):
    level = steps_of(rng, dims, pieces, -0.22, 0.18) if pieces else 1.0
    values = jax.random.normal(rng, dims, jnp.float32) * deviation * level
    return jnp.minimum(jnp.maximum(values, -limit), limit).astype(kind)


def setup_inputs(seed: int = 0, part: int = 0) -> dict:
    streams_of = jax.random.split(jax.random.key(seed), 13)
    part_splits = jax.random.split(jax.random.fold_in(streams_of[12], part), 13)
    hidden = draw_hidden(jax.random.fold_in(jax.random.fold_in(streams_of[12], part), 71), part)
    attention_gain = jnp.clip(1.0 + 0.15 * jax.random.normal(streams_of[1], (MODEL_WIDTH,), jnp.float32), 0.25, 1.75)
    query_weight = noise(streams_of[2], (MODEL_WIDTH, QUERY_HEADS * HEAD_WIDTH), MODEL_WIDTH ** -0.5, 0.0625, ((0, 4), (1, 4)))
    key_projector = noise(streams_of[3], (MODEL_WIDTH, KEY_VALUE_HEADS * HEAD_WIDTH), MODEL_WIDTH ** -0.5, 0.0625, ((0, 4), (1, 4)))
    value_projector = noise(streams_of[4], (MODEL_WIDTH, KEY_VALUE_HEADS * HEAD_WIDTH), MODEL_WIDTH ** -0.5, 0.0625, ((0, 4), (1, 4)))
    out_weight = noise(streams_of[5], (QUERY_HEADS * HEAD_WIDTH, MODEL_WIDTH), (QUERY_HEADS * HEAD_WIDTH // 9) ** -0.5, 0.1875, ((0, 4), (1, 4)))
    key_cache = draw_key_cache(jax.random.fold_in(jax.random.fold_in(streams_of[12], part), 71), part)
    earlier_value_cache = noise(part_splits[7], (SEQUENCE_COUNT, KEY_VALUE_HEADS, CACHE_SLOTS, HEAD_WIDTH), 1.0, 6.0, ((0, 4), (1, 4)))
    cached_length_per_row = set_ends(jax.random.randint(part_splits[8], (SEQUENCE_COUNT,), 1, CACHE_SLOTS + 1), jax.random.fold_in(part_splits[8], 1), 1, CACHE_SLOTS).astype(jnp.int32)
    final_gain = jnp.clip(1.0 + 0.15 * jax.random.normal(streams_of[9], (MODEL_WIDTH,), jnp.float32), 0.25, 1.75)
    head_weight = draw_head_weight(jax.random.fold_in(streams_of[12], 71), part)
    draft_ids = set_ends(jax.random.randint(part_splits[11], (SEQUENCE_COUNT,), 0, VOCAB), jax.random.fold_in(part_splits[11], 1), 0, VOCAB - 1).astype(jnp.int32)
    return dict(hidden=hidden, attention_gain=attention_gain, query_weight=query_weight, key_projector=key_projector, value_projector=value_projector, out_weight=out_weight, key_cache=key_cache, earlier_value_cache=earlier_value_cache, cached_length_per_row=cached_length_per_row, final_gain=final_gain, head_weight=head_weight, draft_ids=draft_ids)


EPSILON = 1e-05
THETA = 10000.0

def rotary_embedding(vectors, positions):
    half_dim = vectors.shape[-1] // 2
    frequency = THETA ** (-2.0 * jnp.arange(half_dim, dtype=jnp.float32) / vectors.shape[-1])
    angles = positions.astype(jnp.float32)[:, None, None] * frequency[None, None, :]
    cosine = jnp.cos(angles)
    sine_part = jnp.sin(angles)
    former = vectors[..., :half_dim]
    latter = vectors[..., half_dim:]
    return jnp.concatenate([former * cosine - latter * sine_part, latter * cosine + former * sine_part], axis=-1)

def rms_normed(matrix, gain_row):
    wide_rows = matrix.astype(jnp.float32)
    mean_square = lax.optimization_barrier(jnp.mean(wide_rows * wide_rows, axis=-1, keepdims=True))
    return (wide_rows * lax.rsqrt(mean_square + EPSILON) * gain_row).astype(jnp.bfloat16)

def attend(query_rows, key_cache, earlier_value_cache, incoming_key, incoming_value, lengths):
    score_scale = HEAD_WIDTH ** (-0.5)
    scores = jnp.einsum('bgrd,bgtd->bgrt', query_rows.astype(jnp.float32), key_cache.astype(jnp.float32)) * score_scale
    places = lax.broadcasted_iota(jnp.int32, scores.shape, 3)
    scores = jnp.where(places < lengths[:, None, None, None], scores, -jnp.inf)
    own_score = jnp.einsum('bgrd,bgd->bgr', query_rows.astype(jnp.float32), incoming_key.astype(jnp.float32)) * score_scale
    highest = jnp.maximum(lax.optimization_barrier(jnp.max(scores, axis=3)), own_score)
    exponent = jnp.exp(scores - highest[..., None])
    own_exp = jnp.exp(own_score - highest)
    denominator = lax.optimization_barrier(jnp.sum(exponent, axis=3)) + own_exp
    weights = lax.optimization_barrier(exponent.astype(jnp.bfloat16)).astype(jnp.float32)
    own_weight = lax.optimization_barrier(own_exp.astype(jnp.bfloat16)).astype(jnp.float32)
    numerator = jnp.einsum('bgrt,bgtd->bgrd', weights, earlier_value_cache.astype(jnp.float32))
    numerator = numerator + own_weight[..., None] * incoming_value.astype(jnp.float32)[:, :, None, :]
    return (numerator / denominator[..., None]).astype(jnp.bfloat16)

def reference(hidden, attention_gain, query_weight, key_projector, value_projector, out_weight, key_cache, earlier_value_cache, cached_length_per_row, final_gain, head_weight, draft_ids):
    normed_in = rms_normed(hidden, attention_gain)
    query_raw = jnp.dot(normed_in, query_weight, preferred_element_type=jnp.float32)
    unrotated_key = jnp.dot(normed_in, key_projector, preferred_element_type=jnp.float32)
    projected_value = jnp.dot(normed_in, value_projector, preferred_element_type=jnp.float32)
    query_rows = rotary_embedding(query_raw.reshape(SEQUENCE_COUNT, QUERY_HEADS, HEAD_WIDTH), cached_length_per_row).astype(jnp.bfloat16)
    query_rows = query_rows.reshape(SEQUENCE_COUNT, KEY_VALUE_HEADS, QUERY_HEADS // KEY_VALUE_HEADS, HEAD_WIDTH)
    incoming_key = rotary_embedding(unrotated_key.reshape(SEQUENCE_COUNT, KEY_VALUE_HEADS, HEAD_WIDTH), cached_length_per_row).astype(jnp.bfloat16)
    incoming_value = projected_value.reshape(SEQUENCE_COUNT, KEY_VALUE_HEADS, HEAD_WIDTH).astype(jnp.bfloat16)
    mixed = attend(query_rows, key_cache, earlier_value_cache, incoming_key, incoming_value, cached_length_per_row).reshape(SEQUENCE_COUNT, QUERY_HEADS * HEAD_WIDTH)
    attention_out = jnp.dot(mixed, out_weight, preferred_element_type=jnp.float32)
    residual_out = (hidden.astype(jnp.float32) + attention_out).astype(jnp.bfloat16)
    normed_out = rms_normed(residual_out, final_gain)
    logits = jnp.dot(normed_out, head_weight.T, preferred_element_type=jnp.float32)
    highest = lax.optimization_barrier(jnp.max(logits, axis=1))
    log_total = highest + jnp.log(lax.optimization_barrier(jnp.sum(jnp.exp(logits - highest[:, None]), axis=1)))
    target_logit = jnp.take_along_axis(logits, draft_ids[:, None].astype(jnp.int32), axis=1)[:, 0]
    return (residual_out, target_logit - log_total)
```

```python
import functools
import math

import jax
import jax.numpy as jnp
from jax import lax
from jax.experimental import pallas as pl
from jax.experimental.pallas import tpu as pltpu
from jax.sharding import PartitionSpec as P

EPSILON = 1e-05
THETA = 10000.0
LANES = 128
MESH = pl.DeviceIdType.MESH
F32 = jnp.float32
BF16 = jnp.bfloat16
WINDOWS = (2, 2, 1, 2)
REST_WINDOW = 2
VMEM_BYTES = 62 * 1024 * 1024


def each(first, last, body):
    if last - first <= 16:
        for k in range(first, last):
            body(k)
    else:

        @pl.loop(first, last)
        def _(k):
            body(k)


def aligned(start):
    return start if isinstance(start, int) else pl.multiple_of(start, LANES)


BLOCK = 256


def halves(columns):
    if columns % (4 * LANES):
        return [(0, columns)]
    return [(0, columns // 2), (columns // 2, columns // 2)]


def kernel(
    n_dp, n_mp, chunk, windows,
    hidden, attention_gain, query_weight, key_projector, value_projector, out_weight,
    key_cache, value_cache, lengths_in, final_gain, head_weight, ids_in,
    residual_out, logprob_out,
    hid_v, gain_v, wq_v, wk_v, wv_v, wo_v, kc_v, vc_v, fgain_v, head_v,
    x_recv, x_v, sum_send, sum_recv, proj_send, proj_recv, mix_send, mix_recv, mix_v,
    att_send, att_recv, own_send, own_recv, res_send, res_sent, res_recv, ss_send, ss_recv, y_v,
    log_send, log_recv, fin_send, fin_recv, lengths, draft_ids,
    load_sem, head_sem,
    x_ss, x_rs, sum_ss, sum_rs, proj_ss, proj_rs, mix_ss, mix_rs, att_ss, att_rs,
    own_ss, own_rs, res_ss, res_rs, ss_ss, ss_rs, log_ss, log_rs, fin_ss, fin_rs,
):
    j = lax.axis_index("dp")
    i = lax.axis_index("mp")
    count = n_dp * n_mp
    me = j * n_mp + i
    rows, width = hid_v.shape
    model_width = width * n_dp
    sequences, pairs, slots, head_size = kc_v.shape
    query_cols = wq_v.shape[1]
    pair_cols = wk_v.shape[1]
    group = query_cols // pair_cols
    quarter = y_v.shape[1]
    blocks = quarter // width
    vocab = head_v.shape[0]
    chunks = log_send.shape[0]
    full = vocab // chunk
    rest = vocab - full * chunk
    even = chunk % BLOCK == 0 and quarter % BLOCK == 0
    plan = []
    for w, number in enumerate(windows):
        first = sum(windows[:w])
        mine = [c for c in range(first, first + number) if c < full]
        if w == REST_WINDOW and rest >= BLOCK:
            mine.append(full)
        plan.append(mine if even else [])
    order = [c for mine in plan for c in mine]
    turned = set(order)
    order += [c for c in range(chunks) if c not in turned]

    far_half = j // ((n_dp + 1) // 2)
    reach = jnp.maximum(j, n_dp - 1 - j)

    def far(k):
        step = (k - 1) + (k - 1) // reach
        return far_half * step + (1 - far_half) * (n_dp - 1 - step)

    def everyone(action):
        def along(k):
            for step in range(n_mp):
                action(far(k), lax.rem(i + step, n_mp))

        each(1, n_dp, along)
        for step in range(1, n_mp):
            action(j, lax.rem(i + step, n_mp))

    def load(source, target, slot):
        copy = pltpu.make_async_copy(source, target, load_sem.at[slot])
        copy.start()
        return copy

    hid_in = load(hidden, hid_v, 0)
    barrier = pltpu.get_barrier_semaphore()
    everyone(
        lambda dp, mp: pl.semaphore_signal(
            barrier, inc=1, device_id={"dp": dp, "mp": mp}, device_id_type=MESH
        )
    )

    gain_in = load(attention_gain, gain_v, 1)
    len_in = load(lengths_in, lengths, 9)
    ids_load = load(ids_in, draft_ids, 10)
    wk_in = load(key_projector, wk_v, 2)
    wv_in = load(value_projector, wv_v, 3)
    wq_in = load(query_weight, wq_v, 4)
    kc_in = load(key_cache, kc_v, 5)
    vc_in = load(value_cache, vc_v, 6)

    def head_copy(c):
        size = chunk if c < full else vocab - full * chunk
        return pltpu.make_async_copy(
            head_weight.at[pl.ds(c * chunk, size)], head_v.at[pl.ds(c * chunk, size)], head_sem.at[c]
        )

    def remote(source, target, send, receive, device):
        return pltpu.make_async_remote_copy(
            src_ref=source, dst_ref=target, send_sem=send, recv_sem=receive,
            device_id=device, device_id_type=MESH,
        )

    def x_copy(k):
        return remote(
            hid_v, x_recv.at[i], x_ss, x_rs, {"dp": j, "mp": lax.rem(i + k, n_mp)}
        )

    def finished(copies, buffer, sem):
        if copies:
            pltpu.make_async_copy(
                buffer.at[pl.ds(0, copies)], buffer.at[pl.ds(0, copies)], sem
            ).wait()

    def sum_copy(dp, mp):
        return remote(
            sum_send, sum_recv.at[me], sum_ss, sum_rs, {"dp": dp, "mp": mp}
        )

    hid_in.wait()
    own = hid_v[...].astype(F32)
    sum_send[...] = jnp.broadcast_to(jnp.sum(own * own, axis=1, keepdims=True), sum_send.shape)
    sum_recv[me] = sum_send[...]
    x_recv[i] = hid_v[...]
    pl.semaphore_wait(barrier, count - 1)
    everyone(lambda dp, mp: sum_copy(dp, mp).start())
    each(1, n_mp, lambda k: x_copy(k).start())
    wo_in = load(out_weight, wo_v, 7)
    len_in.wait()
    lane = lax.broadcasted_iota(jnp.int32, (1, head_size), 1)
    half = head_size // 2
    index = jnp.where(lane < half, lane, lane - half).astype(F32)
    frequency = jnp.exp(index * (-2.0 * math.log(THETA) / head_size))
    turns = []
    for s in range(sequences):
        angles = lengths[s].astype(F32) * frequency
        sine = jnp.sin(angles)
        turns.append((jnp.cos(angles), jnp.where(lane < half, -sine, sine)))
    gain_in.wait()
    gain = gain_v[...]

    def scale_of(squares):
        return lax.rsqrt(squares / model_width + EPSILON)

    finished(n_mp - 1, x_recv, x_rs)
    for c in order[:3]:
        head_copy(c).start()
    wk_in.wait()
    wv_in.wait()
    wq_in.wait()
    finished(count - 1, sum_recv, sum_rs)
    normed = []
    for r in range(n_mp):
        squares = sum_recv[r]
        for d in range(1, n_dp):
            squares += sum_recv[d * n_mp + r]
        normed.append(x_recv[r].astype(F32) * scale_of(squares[:, :1]) * gain)
    x_v[...] = jnp.concatenate(normed, axis=0).astype(BF16)

    def proj_copy(k, start, size):
        t = far(k)
        lanes = pl.ds(start, size)
        return remote(
            proj_send.at[t, :, lanes], proj_recv.at[j, :, lanes], proj_ss, proj_rs,
            {"dp": t, "mp": i},
        )

    def proj_out(parts):
        first = parts[0][0]
        last = first
        for start, part in parts:
            last = start + part.shape[1]
            for t in range(n_dp):
                proj_send[t, :, start:last] = part[t * sequences : (t + 1) * sequences]
        each(1, n_dp, lambda k: proj_copy(k, first, last - first).start())

    def piece(left, weight, start, size):
        return jnp.dot(left[...], weight[:, start : start + size], preferred_element_type=F32)

    held = None
    for start, size in halves(query_cols):
        part = piece(x_v, wq_v, start, size)
        if held is not None:
            proj_out(held)
        held = [(start, part)]
    tail = [
        (query_cols, piece(x_v, wk_v, 0, pair_cols)),
        (query_cols + pair_cols, piece(x_v, wv_v, 0, pair_cols)),
    ]
    proj_out(held)
    proj_out(tail)
    fgain_in = load(
        final_gain.at[:, pl.ds(pl.multiple_of(i * quarter, LANES), quarter)], fgain_v, 8
    )
    for c in order[3:]:
        head_copy(c).start()
    kc_in.wait()
    vc_in.wait()
    proj_recv[j] = proj_send[j]

    def turn(start, blocks):
        for p in range(0, blocks * BLOCK, BLOCK):
            for k in range(0, quarter, BLOCK):
                spot = (pl.ds(start + p, BLOCK), slice(k, k + BLOCK))
                head_v[spot] = head_v[spot].T

    def use_window(w):
        for c in plan[w]:
            head_copy(c).wait()
            turn(c * chunk, (chunk if c < full else rest) // BLOCK)

    use_window(0)
    finished(n_dp - 1, proj_recv, proj_rs)
    projected = proj_recv[0]
    for d in range(1, n_dp):
        projected += proj_recv[d]

    def rotated(vectors, turn):
        swapped = jnp.concatenate([vectors[:, half:], vectors[:, :half]], axis=1)
        return (vectors * turn[0] + swapped * turn[1]).astype(BF16)

    scale = head_size ** (-0.5)
    for s in range(sequences):
        def heads_of(start, number):
            return jnp.concatenate(
                [
                    projected[s : s + 1, start + h * head_size : start + (h + 1) * head_size]
                    for h in range(number)
                ],
                axis=0,
            )

        queries = rotated(heads_of(0, pairs * group), turns[s])
        keys = rotated(heads_of(query_cols, pairs), turns[s])
        values = heads_of(query_cols + pair_cols, pairs).astype(BF16)
        mixed = []
        for g in range(pairs):
            query = queries[g * group : (g + 1) * group]
            own_score = scale * jnp.sum(
                query.astype(F32) * keys[g : g + 1].astype(F32), axis=1, keepdims=True
            )
            scores = scale * lax.dot_general(
                query, kc_v[s, g], (((1,), (1,)), ((), ())), preferred_element_type=F32
            )
            spots = lax.broadcasted_iota(jnp.int32, scores.shape, 1)
            scores = jnp.where(spots < lengths[s], scores, -jnp.inf)
            highest = jnp.maximum(jnp.max(scores, axis=1, keepdims=True), own_score)
            exponent = jnp.exp(scores - highest)
            own_exp = jnp.exp(own_score - highest)
            denominator = jnp.sum(exponent, axis=1, keepdims=True) + own_exp
            numerator = jnp.dot(exponent.astype(BF16), vc_v[s, g], preferred_element_type=F32)
            numerator += own_exp.astype(BF16).astype(F32) * values[g : g + 1].astype(F32)
            mixed.append(numerator / denominator)
        mixed = [m[h : h + 1] for m in mixed for h in range(group)]
        mix_send[s : s + 1] = jnp.concatenate(mixed, axis=1).astype(BF16)

    def mix_copy(k):
        return remote(
            mix_send, mix_recv.at[j], mix_ss, mix_rs, {"dp": far(k), "mp": i},
        )

    each(1, n_dp, lambda k: mix_copy(k).start())
    mix_recv[j] = mix_send[...]
    wo_in.wait()
    use_window(1)
    finished(n_dp - 1, mix_recv, mix_rs)
    mix_v[...] = jnp.concatenate(
        [mix_recv[d].astype(F32) for d in range(n_dp)], axis=0
    ).astype(BF16)

    reader = j // blocks
    spot = lax.rem(j, blocks)

    def att_copy(start, size):
        lanes = pl.ds(start, size)
        return remote(
            att_send.at[:, lanes], att_recv.at[i, :, lanes], att_ss, att_rs,
            {"dp": j, "mp": reader},
        )

    def att_out(start, part):
        size = part.shape[1]
        att_send[:, start : start + size] = part

        @pl.when(reader != i)
        def _():
            att_copy(start, size).start()

    held = None
    for start, size in halves(width):
        part = piece(mix_v, wo_v, start, size)
        if held is not None:
            att_out(*held)
        held = (start, part)
    att_out(*held)
    use_window(2)

    def res_copy(dp):
        return remote(res_send, res_recv.at[spot], res_ss, res_rs, {"dp": dp, "mp": i})

    def own_copy(k):
        t = lax.rem(i + k, n_mp)
        return remote(own_send.at[t], own_recv, own_ss, own_rs, {"dp": j, "mp": t})

    @pl.when(reader == i)
    def _():
        attended = att_send[...] + jnp.concatenate(
            [x_recv[r].astype(F32) for r in range(n_mp)], axis=0
        )
        finished(n_mp - 1, att_recv, att_rs)
        for k in range(1, n_mp):
            attended += att_recv[lax.rem(i + k, n_mp)]
        residual = attended.astype(BF16)
        res_send[...] = residual
        each(1, n_dp, lambda k: res_copy(far(k)).start())
        res_recv[spot] = residual
        for r in range(n_mp):
            own_send[r] = residual[r * rows : (r + 1) * rows]
        each(1, n_mp, lambda k: own_copy(k).start())
        residual_out[...] = own_send[i]

    ids_load.wait()
    ids = jnp.zeros((rows, 1), jnp.int32)
    row_index = lax.broadcasted_iota(jnp.int32, (rows, 1), 0)
    for r in range(rows):
        ids = jnp.where(row_index == r, draft_ids[r], ids)
    fgain_in.wait()
    final = fgain_v[...]
    use_window(3)

    @pl.when(reader == i)
    def _():
        finished(blocks - 1, res_recv, res_rs)

    @pl.when(reader != i)
    def _():
        finished(blocks, res_recv, res_rs)

    wides = jnp.concatenate([res_recv[b].astype(F32) for b in range(blocks)], axis=1)
    y_v[...] = (wides * final).astype(BF16)
    squares = jnp.sum(wides * wides, axis=1, keepdims=True)
    for r in range(n_mp):
        ss_send[r] = jnp.broadcast_to(squares[r * rows : (r + 1) * rows], (rows, LANES))

    def ss_copy(k):
        t = lax.rem(i + k, n_mp)
        return remote(ss_send.at[t], ss_recv.at[i], ss_ss, ss_rs, {"dp": j, "mp": t})

    def log_copy(c, k):
        t = lax.rem(i + k, n_mp)
        return remote(
            log_send.at[c, t], log_recv.at[c, i], log_ss.at[c], log_rs.at[c],
            {"dp": j, "mp": t},
        )

    def keep_logits(c, parts):
        for p, part in parts:
            for t in range(n_mp):
                log_send[c, t, :, p : p + part.shape[1]] = part[t * rows : (t + 1) * rows]

    def head_chunk(c):
        size = chunk if c < full else rest
        ready = size // BLOCK * BLOCK if c in turned else 0
        if c not in turned:
            head_copy(c).wait()
        parts = []
        for p in range(0, ready, BLOCK):
            part = None
            for k in range(0, quarter, BLOCK):
                one = jnp.dot(
                    y_v[:, k : k + BLOCK], head_v[pl.ds(c * chunk + p, BLOCK), k : k + BLOCK],
                    preferred_element_type=F32,
                )
                part = one if part is None else part + one
            parts.append((p, part))
        for p in range(ready, size, BLOCK):
            part = lax.dot_general(
                y_v[...], head_v[pl.ds(c * chunk + p, min(BLOCK, size - p))],
                (((1,), (1,)), ((), ())), preferred_element_type=F32,
            )
            parts.append((p, part))
        return parts

    each(1, n_mp, lambda k: ss_copy(k).start())
    if rest:
        log_send[full, :, :, rest // LANES * LANES :] = jnp.zeros(
            (n_mp, rows, chunk - rest // LANES * LANES), F32
        )
    for at, c in enumerate(order):
        parts = head_chunk(c)
        if at:
            each(1, n_mp, lambda k: log_copy(order[at - 1], k).start())
        keep_logits(c, parts)
    each(1, n_mp, lambda k: log_copy(order[-1], k).start())

    finished(n_mp - 1, ss_recv, ss_rs)
    squares = ss_send[i]
    for k in range(1, n_mp):
        squares += ss_recv[lax.rem(i + k, n_mp)]
    scales = scale_of(squares[:, :1])
    column = lax.broadcasted_iota(jnp.int32, (rows, chunk), 1)

    def stats(group):
        pieces, target, peak = [], jnp.zeros((rows, chunk), F32), None
        for c in group:
            logits = log_send[c, i]
            finished(n_mp - 1, log_recv.at[c], log_rs.at[c])
            for k in range(1, n_mp):
                logits += log_recv[c, lax.rem(i + k, n_mp)]
            logits = logits * scales
            here = ids - (c * chunk + j * vocab)
            if c >= full:
                logits = jnp.where(column < rest, logits, -jnp.inf)
                here = jnp.where(here < rest, here, -1)
            target = jnp.where(column == here, logits, target)
            pieces.append(logits)
            peak = logits if peak is None else jnp.maximum(peak, logits)
        peak = jnp.max(peak, axis=1, keepdims=True)
        mass = sum(jnp.exp(piece - peak) for piece in pieces)
        return peak, jnp.sum(mass, axis=1, keepdims=True), jnp.sum(target, axis=1, keepdims=True)

    early = stats(order[:-1]) if chunks > 1 else None
    peak, mass, target = stats(order[-1:])
    if early is not None:
        early_peak, early_mass, early_target = early
        top = jnp.maximum(peak, early_peak)
        mass = mass * jnp.exp(peak - top) + early_mass * jnp.exp(early_peak - top)
        peak, target = top, target + early_target
    for p, value in enumerate((peak, mass, target)):
        fin_send[p] = jnp.broadcast_to(value, (rows, LANES))

    def fin_copy(k):
        return remote(
            fin_send, fin_recv.at[j], fin_ss, fin_rs,
            {"dp": far(k), "mp": i},
        )

    each(1, n_dp, lambda k: fin_copy(k).start())
    fin_recv[j] = fin_send[...]

    finished(n_mp - 1, x_recv, x_ss)
    finished(count - 1, sum_recv, sum_ss)
    finished(n_dp - 1, proj_recv, proj_ss)
    finished(n_dp - 1, mix_recv, mix_ss)

    @pl.when(reader == i)
    def _():
        finished(n_dp - 1, res_sent, res_ss)
        finished(n_mp - 1, own_send, own_ss)

    @pl.when(reader != i)
    def _():
        pltpu.make_async_copy(att_send, att_send, att_ss).wait()
        pltpu.make_async_copy(own_recv, own_recv, own_rs).wait()
        residual_out[...] = own_recv[...]

    finished(n_mp - 1, ss_recv, ss_ss)
    for c in range(chunks):
        finished(n_mp - 1, log_recv.at[c], log_ss.at[c])
    finished(n_dp - 1, fin_recv, fin_rs)
    finished(n_dp - 1, fin_recv, fin_ss)

    tiles = [fin_recv[d] for d in range(n_dp)]
    overall = tiles[0][0]
    for tile in tiles[1:]:
        overall = jnp.maximum(overall, tile[0])
    mass = jnp.zeros_like(overall)
    target = jnp.zeros_like(overall)
    for tile in tiles:
        mass += tile[1] * jnp.exp(tile[0] - overall)
        target += tile[2]
    logprob_out[...] = target - (overall + jnp.log(mass))


def deliver(residual, logprob, residual_out, logprob_out):
    residual_out[...] = residual[...]
    for r in range(logprob.shape[0]):
        logprob_out[r] = logprob[r, 0]


def solution(mesh):
    n_dp, n_mp = mesh.shape["dp"], mesh.shape["mp"]

    def shards(
        hidden, attention_gain, query_weight, key_projector, value_projector, out_weight,
        key_cache, earlier_value_cache, cached_length_per_row, final_gain, head_weight, draft_ids,
    ):
        rows, width = hidden.shape
        sequences = key_cache.shape[0]
        query_cols = query_weight.shape[1]
        wide = query_cols + key_projector.shape[1] + value_projector.shape[1]
        vocab, quarter = head_weight.shape
        chunk = min(1024, -(-vocab // LANES) * LANES)
        chunks = -(-vocab // chunk)
        blocks = quarter // width
        count = n_dp * n_mp
        vmem, dma, smem = pltpu.VMEM, pltpu.SemaphoreType.DMA, pltpu.SMEM
        flat = (1, width)
        scratch = [
            vmem(hidden.shape, BF16), vmem(flat, F32),
            *[vmem(w.shape, BF16) for w in (query_weight, key_projector, value_projector, out_weight)],
            vmem(key_cache.shape, BF16), vmem(earlier_value_cache.shape, BF16),
            vmem((1, quarter), F32), vmem(head_weight.shape, BF16),
            vmem((n_mp, rows, width), BF16), vmem((n_mp * rows, width), BF16),
            vmem((rows, LANES), F32), vmem((count, rows, LANES), F32),
            vmem((n_dp, sequences, wide), F32), vmem((n_dp, sequences, wide), F32),
            vmem((sequences, query_cols), BF16), vmem((n_dp, sequences, query_cols), BF16),
            vmem((n_dp * sequences, query_cols), BF16),
            vmem((n_mp * rows, width), F32), vmem((n_mp, n_mp * rows, width), F32),
            vmem((n_mp, rows, width), BF16), vmem((rows, width), BF16),
            vmem((n_mp * rows, width), BF16), vmem((n_dp, n_mp * rows, width), BF16),
            vmem((blocks, n_mp * rows, width), BF16),
            vmem((n_mp, rows, LANES), F32), vmem((n_mp, rows, LANES), F32),
            vmem((n_mp * rows, quarter), BF16),
            vmem((chunks, n_mp, rows, chunk), F32), vmem((chunks, n_mp, rows, chunk), F32),
            vmem((3, rows, LANES), F32), vmem((n_dp, 3, rows, LANES), F32),
            smem(cached_length_per_row.shape, jnp.int32), smem(draft_ids.shape, jnp.int32),
            dma((11,)), dma((chunks,)),
            *[dma] * 16, dma((chunks,)), dma((chunks,)), dma, dma,
        ]
        anywhere = pl.BlockSpec(memory_space=pl.ANY)
        far = pl.BlockSpec(memory_space=pltpu.HBM)
        inside = pl.BlockSpec(memory_space=pltpu.VMEM)
        scalars = pl.BlockSpec(memory_space=pltpu.SMEM)
        residual, logprob = pl.pallas_call(
            functools.partial(kernel, n_dp, n_mp, chunk, WINDOWS),
            out_shape=(vmem(hidden.shape, BF16), vmem((rows, LANES), F32)),
            in_specs=[anywhere] * 8 + [far] + [anywhere] * 2 + [far],
            out_specs=(inside, inside),
            scratch_shapes=scratch,
            compiler_params=pltpu.CompilerParams(
                collective_id=0, has_side_effects=True, vmem_limit_bytes=VMEM_BYTES
            ),
        )(
            hidden, attention_gain.reshape(flat), query_weight, key_projector, value_projector,
            out_weight, key_cache, earlier_value_cache, cached_length_per_row,
            final_gain.reshape(1, -1), head_weight, draft_ids,
        )
        return pl.pallas_call(
            deliver,
            out_shape=(
                jax.ShapeDtypeStruct(hidden.shape, BF16),
                jax.ShapeDtypeStruct(draft_ids.shape, F32),
            ),
            in_specs=[inside, inside],
            out_specs=(inside, scalars),
        )(
            pltpu.with_memory_space_constraint(residual, vmem),
            pltpu.with_memory_space_constraint(logprob, vmem),
        )

    in_specs = (
        P(("groups", "mp"), "dp"),
        P("dp"),
        P("dp", "mp"),
        P("dp", "mp"),
        P("dp", "mp"),
        P("mp", "dp"),
        P(("groups", "dp"), "mp", None, None),
        P(("groups", "dp"), "mp", None, None),
        P(("groups", "dp")),
        P(),
        P("dp", "mp"),
        P(("groups", "mp")),
    )
    out_specs = (P(("groups", "mp"), "dp"), P(("groups", "mp")))
    return jax.shard_map(shards, mesh=mesh, in_specs=in_specs, out_specs=out_specs, check_vma=False)
```
